32 devices in a mesh: gx: 4 (over z), gy: 8 (over y, x, core).
Axes of the slice: x: 2, y: 2, z: 4, core: 2. Of those that a mesh axis runs over, the one named last changes fastest.
Arguments:
- tokens: bfloat16 [28672, 4096], P(('gx', 'gy')), may hold values from -6 to 6
- codes: bfloat16 [4096, 512], P(('gx', 'gy')), may hold values from -0.09375 to 0.09375
- scales: float32 [128, 4], P(('gx', 'gy')), may hold values from 0.5 to 2
- gain: float32 [128], replicated, may hold values from 0.1 to 1.9
- cotangent: bfloat16 [28672, 512], P(('gx', 'gy')), may hold values from -96 to 96
Outputs:
- keys: bfloat16 [28672, 512], P(('gx', 'gy'))
- token_grad: bfloat16 [28672, 4096], P(('gx', 'gy'))
- weight_grad: float32 [4096, 512], P(('gx', 'gy'))
The draws below stay inside these ranges and needn't reach their ends.
All inputs are finite; a program needn't handle non-finite values.
Results may differ from the reference program's by a relative error of at most 0.019.
Values may be sent and summed in bfloat16 or wider, within the bound.
No kernel may reach another device: no remote copies, remote signals or barrier semaphores. Data moves between devices by JAX's collectives and lax.ppermute only.
A program may use at most 128 MiB of HBM per device.

```python
import math
import jax
import jax.numpy as jnp
from jax import lax

D = 4096
KV_HEADS = 4
HEAD = 128
QBLK = 32
TOK_DEV = 896
KV = 512
TOKENS = 28672
N_GX = 4
N_GY = 8


def draw_cotangent(key, part):
    pick_key, boost_key, value_key = jax.random.split(key, 3)
    columns = jnp.arange(HEAD, dtype=jnp.int32)
    marked = []
    for head_index in range(KV_HEADS):
        picked = jax.random.permutation(jax.random.fold_in(pick_key, head_index), HEAD)
        marked.append(jnp.logical_or(columns == picked[0], columns == picked[1]))
    chosen = jnp.concatenate(marked).astype(jnp.float32)
    boost_scale = jax.random.uniform(boost_key, (KV,), jnp.float32, 8.0, 16.0)
    column_scale = 1.0 + chosen * (boost_scale - 1.0)
    values = jax.random.truncated_normal(value_key, -6.0, 6.0, (TOKENS, KV), jnp.float32)
    return (values * column_scale[None, :]).astype(jnp.bfloat16)


def strengthened(drawn, key, source, target, blocks, factor):
    owner, partner = [(jnp.arange(drawn.shape[dim]) // (drawn.shape[dim] // blocks)).reshape([-1 if axis == dim else 1 for axis in range(drawn.ndim)]) for dim in (source, target)]
    chosen = jax.random.permutation(key, blocks)[partner]
    strong = (owner == chosen) | (owner == (partner + blocks // 2) % blocks)
    return jnp.where(strong, factor * drawn, drawn)


def block_levels(rng, dims, cuts, least, high):
    level = 1.0
    for dim, blocks in cuts:
        draws = jax.random.uniform(jax.random.fold_in(jax.random.fold_in(rng, 6), dim), (blocks,), jnp.float32, least / len(cuts), high / len(cuts))
        level = level * jnp.repeat(jnp.exp(draws), dims[dim] // blocks).reshape((-1,) + (1,) * (len(dims) - 1 - dim))
    return level


def normal_values(own_key, dims, scale, bound, pieces=(), kind=jnp.bfloat16):
    result = scale * jax.random.normal(own_key, dims, jnp.float32)
    if pieces:
        result = result * block_levels(own_key, dims, pieces, -0.22, 0.18)
    return jnp.clip(result, -bound, bound).astype(kind)


def bell_draw_with(stream_key, shape, spread, limit, shards, heavy, kind=jnp.bfloat16):
    values = spread * jax.random.normal(stream_key, shape, jnp.float32)
    if shards:
        values = values * block_levels(stream_key, shape, shards, -0.22, 0.18)
    return jnp.clip(strengthened(values, jax.random.fold_in(stream_key, 3), *heavy), -limit, limit).astype(kind)


def setup_inputs(seed: int = 0) -> dict:
    seeds = jax.random.split(jax.random.key(seed), 6)
    return {
        "tokens": bell_draw_with(seeds[0], (TOKENS, D), 1.0, 6.0, ((0, 32),), (0, 1, 32, 2.75)),
        "codes": normal_values(seeds[1], (D, KV), D ** -0.5, 0.09375, ((0, 32),)),
        "scales": jnp.clip(jnp.exp(math.log(2.0) - 1.3862944 * jax.random.uniform(seeds[2], (D // QBLK, KV_HEADS), jnp.float32) ** block_levels(seeds[2], (D // QBLK, KV_HEADS), ((0, 32),), -0.2, 0.2)), 0.5, 2.0),
        "gain": jnp.clip(1.0 + 0.18 * jax.random.normal(seeds[3], (HEAD,), jnp.float32), 0.1, 1.9),
        "cotangent": draw_cotangent(jax.random.fold_in(seeds[5], 71), 0),
    }


clip_ratio = 2.5

def hadamard(length):
    indices = jnp.arange(length, dtype=jnp.int32)
    common = jnp.bitwise_and(indices[:, None], indices[None, :])
    parity = jnp.zeros((length, length), jnp.int32)
    for position in range(length.bit_length() - 1):
        parity = parity + jnp.bitwise_and(jnp.right_shift(common, position), 1)
    return (1 - 2 * (parity % 2)).astype(jnp.float32) / math.sqrt(length)

def rotate(matrix, rotation):
    shaped = matrix.reshape(matrix.shape[0], KV_HEADS, HEAD)
    rotated = jnp.einsum('rhc,cd->rhd', shaped, rotation, precision=lax.Precision.HIGHEST)
    return rotated.reshape(matrix.shape)

def clipped(matrix):
    shaped = matrix.reshape(matrix.shape[0] // QBLK, QBLK, KV_HEADS, HEAD)
    mean_square = lax.optimization_barrier(jnp.mean(shaped * shaped, axis=(1, 3), keepdims=True))
    clip_bound = clip_ratio * jnp.sqrt(mean_square + 1e-06)
    return jnp.clip(shaped, -clip_bound, clip_bound).reshape(matrix.shape)

def normed_keys(projected, gain):
    shaped = projected.reshape(projected.shape[0], KV_HEADS, HEAD)
    mean_square = lax.optimization_barrier(jnp.mean(shaped * shaped, axis=-1, keepdims=True))
    return (shaped * lax.rsqrt(mean_square + 1e-06) * gain).reshape(projected.shape)

def reference(tokens, codes, scales, gain, cotangent):
    blocks = codes.astype(jnp.float32).reshape(D // QBLK, QBLK, KV_HEADS, HEAD)
    weight = (blocks * scales[:, None, :, None]).reshape(D, KV).astype(jnp.bfloat16)
    projected = jnp.dot(tokens, weight, preferred_element_type=jnp.float32)
    normed, pullback = jax.vjp(lambda value_in: normed_keys(value_in, gain), projected)
    keys_out = normed.astype(jnp.bfloat16)
    key_grad = pullback(cotangent.astype(jnp.float32))[0].astype(jnp.bfloat16)
    token_grad = jnp.dot(key_grad, weight.T, preferred_element_type=jnp.float32).astype(jnp.bfloat16)
    rotation = hadamard(HEAD)
    tok_split = tokens.reshape(N_GX, N_GY, TOK_DEV, D)
    grad_split = key_grad.reshape(N_GX, N_GY, TOK_DEV, KV)

    def outer_step(running, outer_index):

        def inner_step(summed, inner_index):
            partial_value = lax.dot_general(tok_split[inner_index, outer_index], grad_split[inner_index, outer_index], (((0,), (0,)), ((), ())), preferred_element_type=jnp.float32)
            coded_term = lax.optimization_barrier(clipped(rotate(partial_value, rotation)).astype(jnp.bfloat16))
            return (summed + coded_term.astype(jnp.float32), None)
        level_one, _ = lax.scan(inner_step, jnp.zeros((D, KV), jnp.float32), jnp.arange(N_GX, dtype=jnp.int32))
        recoded = lax.optimization_barrier(clipped(level_one).astype(jnp.bfloat16))
        return (running + recoded.astype(jnp.float32), None)
    level_two, _ = lax.scan(outer_step, jnp.zeros((D, KV), jnp.float32), jnp.arange(N_GY, dtype=jnp.int32))
    weight_grad = rotate(level_two, rotation)
    return (keys_out, token_grad, weight_grad)
```

```python
import math

import jax
import jax.numpy as jnp
import numpy as np
from jax import lax
from jax.experimental import pallas as pl
from jax.experimental.pallas import tpu as pltpu
from jax.sharding import PartitionSpec as P


HEAD = 128
QBLK = 32
TG_PARTS = 4
CLIP = 2.5
EPS = 1e-06


f32 = jnp.float32
bf16 = jnp.bfloat16
HI = lax.Precision.HIGHEST
BIG = pltpu.CompilerParams(vmem_limit_bytes=60 * 1024 * 1024)


def signs(length):
    idx = np.arange(length)
    common = idx[:, None] & idx[None, :]
    parity = np.zeros((length, length), np.int64)
    for pos in range(length.bit_length() - 1):
        parity += (common >> pos) & 1
    return (1 - 2 * (parity % 2)).astype(np.float32)


def block_mean_matrix(rows):
    lane = np.arange(128)
    return ((lane[:, None] // QBLK) == (lane[None, :] // QBLK)).astype(np.float32) / (QBLK * rows)


def three_parts(x):
    high = x.astype(bf16)
    rest = x - high.astype(f32)
    middle = rest.astype(bf16)
    low = (rest - middle.astype(f32)).astype(bf16)
    return jnp.concatenate([high, middle, low], axis=0)


def clipped_tiles(value, mean_matrix):
    heads = value.shape[0] // HEAD
    groups = value.shape[1] // 128
    tiles = [
        value[h * HEAD : (h + 1) * HEAD, g * 128 : (g + 1) * 128] for h in range(heads) for g in range(groups)
    ]
    rows = [jnp.sum(x * x, axis=0, keepdims=True) for x in tiles]
    pad = -len(rows) % 8
    if pad:
        rows.append(jnp.zeros((pad, 128), f32))
    squares = jnp.concatenate(rows, axis=0)
    count = squares.shape[0]
    parts = jnp.dot(three_parts(squares), mean_matrix, preferred_element_type=f32)
    means = parts[:count] + parts[count : 2 * count] + parts[2 * count :]
    bounds = CLIP * jnp.sqrt(means + EPS)
    for at, x in enumerate(tiles):
        limit = bounds[at : at + 1]
        yield at // groups, at % groups, jnp.minimum(jnp.maximum(x, -limit), limit).astype(bf16)


def scale_kernel(scales_ref, codes_ref, out_ref):
    blocks = codes_ref.shape[0] // QBLK
    heads = codes_ref.shape[1] // HEAD
    for b in range(blocks):
        for h in range(heads):
            tile = codes_ref[b * QBLK : (b + 1) * QBLK, h * HEAD : (h + 1) * HEAD].astype(f32)
            out_ref[b * QBLK : (b + 1) * QBLK, h * HEAD : (h + 1) * HEAD] = (tile * scales_ref[b, h]).astype(bf16)


def scaled(codes, scales):
    return pl.pallas_call(
        scale_kernel,
        out_shape=jax.ShapeDtypeStruct(codes.shape, bf16),
        in_specs=[pl.BlockSpec(memory_space=pltpu.SMEM), pl.BlockSpec(memory_space=pltpu.VMEM)],
        out_specs=pl.BlockSpec(memory_space=pltpu.VMEM),
        name="scale_rows",
    )(scales, codes)


def main_kernel(n, m, r, ra, where_ref, tok_hbm, gain_ref, cot_ref, had_ref, mean_ref, *refs):
    count = m + 2 * n
    pieces = refs[:count]
    keys_ref, kg_ref, qt_ref, term_ref, w_hbm, tv, wv, acc, tsem, wsem, osem = refs[count:]
    gi, gj, side = where_ref[0], where_ref[1], where_ref[2]
    d_model = tv.shape[1]
    heads = acc.shape[1] // HEAD
    kc = 1024
    steps = d_model // kc
    token_copies = [
        pltpu.make_async_copy(tok_hbm.at[:, pl.ds(c * kc, kc)], tv.at[:, pl.ds(c * kc, kc)], tsem.at[c])
        for c in range(steps)
    ]
    weight_copies = []

    def slab(piece, at, a, s, start, length):
        row = lax.rem(gi - a + n, n) * m + jnp.bitwise_xor(gj, s)
        off = pl.multiple_of(row * r + start, 16)
        weight_copies.append(
            pltpu.make_async_copy(piece.at[at], wv.at[pl.ds(off, length)], wsem.at[len(weight_copies)])
        )

    for s in range(m):
        for a in range(n):
            slab(pieces[s], a, a, s, 0, ra)
    for p in range(2 * n):
        for x in range(m // 2):
            slab(pieces[m + p], x, p // 2, 2 * x + p % 2, ra, r - ra)
    for c in weight_copies:
        c.start()
    for c in token_copies:
        c.start()
    for c in weight_copies:
        c.wait()
    w_out = pltpu.make_async_copy(wv, w_hbm, osem)
    w_out.start()
    for c in range(steps):
        token_copies[c].wait()
        part = jnp.dot(tv[:, c * kc : (c + 1) * kc], wv[c * kc : (c + 1) * kc], preferred_element_type=f32)
        if c == 0:
            acc[...] = part
        else:
            acc[...] += part
    gain = gain_ref[...]
    for h in range(heads):
        lanes = slice(h * HEAD, (h + 1) * HEAD)
        raw = acc[:, lanes]
        inv = lax.rsqrt(jnp.mean(raw * raw, axis=-1, keepdims=True) + EPS)
        unit = raw * inv
        keys_ref[:, lanes] = (unit * gain).astype(bf16)
        g = cot_ref[:, lanes].astype(f32) * gain
        kg = (inv * (g - unit * jnp.mean(g * unit, axis=-1, keepdims=True))).astype(bf16)
        kg_ref[:, lanes] = kg
        turned = lax.dot_general(had_ref[...], kg, (((1,), (1,)), ((), ())), preferred_element_type=f32)
        qt_ref[lanes, :] = (turned * (1.0 / math.sqrt(HEAD))).astype(bf16)
    width = term_ref.shape[2]
    bw = min(width, 512)
    for d in range(term_ref.shape[0]):
        row = jnp.where(side == 0, d, n - 1 - d)
        for b in range(width // bw):
            off = pl.multiple_of(row * width + b * bw, bw)
            value = jnp.dot(qt_ref[:HEAD], tv[:, pl.ds(off, bw)], preferred_element_type=f32)
            for _, g, x in clipped_tiles(value, mean_ref[...]):
                term_ref[d, :, b * bw + g * 128 : b * bw + (g + 1) * 128] = x
    w_out.wait()


def main_call(n, m, r, ra, where, tokens, gain, cot, had, mean, pieces):
    tok, d_model = tokens.shape
    kv = cot.shape[1]
    nd = n // 2
    vm = pl.BlockSpec(memory_space=pltpu.VMEM)
    hbm = pl.BlockSpec(memory_space=pltpu.HBM)
    return pl.pallas_call(
        lambda *a: main_kernel(n, m, r, ra, *a),
        out_shape=(
            jax.ShapeDtypeStruct((tok, kv), bf16),
            jax.ShapeDtypeStruct((tok, kv), bf16),
            jax.ShapeDtypeStruct((kv, tok), bf16),
            jax.ShapeDtypeStruct((nd, HEAD, m * r), bf16),
            jax.ShapeDtypeStruct((d_model, kv), bf16),
        ),
        in_specs=[pl.BlockSpec(memory_space=pltpu.SMEM), hbm, vm, vm, vm, vm] + [hbm] * len(pieces),
        out_specs=(vm, vm, vm, vm, hbm),
        scratch_shapes=[
            pltpu.VMEM((tok, d_model), bf16),
            pltpu.VMEM((d_model, kv), bf16),
            pltpu.VMEM((tok, kv), f32),
            pltpu.SemaphoreType.DMA((d_model // 1024,)),
            pltpu.SemaphoreType.DMA((2 * n * m,)),
            pltpu.SemaphoreType.DMA,
        ],
        compiler_params=BIG,
        name="project",
    )(where, tokens, gain, cot, had, mean, *pieces)


def term_kernel(skip, where_ref, tok_ref, qt_ref, mean_ref, *out_refs):
    rows = slice(skip * HEAD, (skip + len(out_refs)) * HEAD)
    value = jnp.dot(qt_ref[rows], tok_ref[...], preferred_element_type=f32)
    for h, g, x in clipped_tiles(value, mean_ref[...]):
        out_refs[h][0, :, g * 128 : (g + 1) * 128] = x


def term_call(n, m, r, where, tokens, qt, mean, first, skip, heads):
    tok = tokens.shape[0]
    kv = qt.shape[0]
    nd = n // 2
    width = m * r
    bw = min(1024, width)
    nb = width // bw

    def tok_index(d, b, where_ref):
        near = where_ref[2] == 0
        row = jnp.where(near if first else jnp.logical_not(near), d, n - 1 - d)
        return (0, row * nb + b)

    return pl.pallas_call(
        lambda *a: term_kernel(skip, *a),
        grid_spec=pltpu.PrefetchScalarGridSpec(
            num_scalar_prefetch=1,
            grid=(nd, nb),
            in_specs=[
                pl.BlockSpec((tok, bw), tok_index),
                pl.BlockSpec((kv, tok), lambda d, b, w: (0, 0)),
                pl.BlockSpec((128, 128), lambda d, b, w: (0, 0)),
            ],
            out_specs=[pl.BlockSpec((1, HEAD, bw), lambda d, b, w: (d, 0, b))] * heads,
        ),
        out_shape=[jax.ShapeDtypeStruct((nd, HEAD, width), bf16)] * heads,
        compiler_params=BIG,
        name="terms",
    )(where, tokens, qt, mean)


def tgrad_kernel(kg_ref, w_ref, *refs):
    refs[-1][...] = lax.dot_general(
        kg_ref[...], w_ref[...], (((1,), (1,)), ((), ())), preferred_element_type=f32
    ).astype(bf16)


def tgrad_call(kg, weight, filled, part, parts):
    tok, kv = kg.shape
    d_model = weight.shape[0]
    bw = 512
    steps = d_model // bw // parts
    base = part * steps
    extra = [] if filled is None else [filled]
    return pl.pallas_call(
        tgrad_kernel,
        grid=(steps,),
        in_specs=[
            pl.BlockSpec((tok, kv), lambda b: (0, 0)),
            pl.BlockSpec((bw, kv), lambda b: (base + b, 0)),
        ] + [pl.BlockSpec(memory_space=pltpu.HBM)] * len(extra),
        out_specs=pl.BlockSpec((tok, bw), lambda b: (0, base + b)),
        out_shape=jax.ShapeDtypeStruct((tok, d_model), bf16),
        input_output_aliases={2: 0} if extra else {},
        compiler_params=BIG,
        name="token_grad",
    )(kg, weight, *extra)


def recode_kernel(aligned, n, where_ref, a_ref, b_ref, mean_ref, keep_ref, send_ref):
    pair, parity = where_ref[1] // 2, lax.rem(where_ref[1], 2)

    @pl.when(jnp.logical_or(where_ref[0] == 0, where_ref[0] == n - 1))
    def _():
        for d in range(a_ref.shape[0]):
            value = a_ref[d].astype(f32) + b_ref[d].astype(f32)
            tiles = [x for _, _, x in clipped_tiles(value, mean_ref[...])]
            for g, x in enumerate(tiles):
                if not aligned:
                    keep_ref[d, :, g * 128 : (g + 1) * 128] = x
                elif g % 2 == 0:
                    at = jnp.bitwise_xor(pair, g // 2)
                    keep_ref[at, d] = jnp.where(parity == 0, x, tiles[g + 1])
                    send_ref[at, d] = jnp.where(parity == 0, tiles[g + 1], x)


def recode_call(n, m, r, where, arrived, mine, mean):
    aligned = r == 128
    vm = pl.BlockSpec(memory_space=pltpu.VMEM)
    nd = arrived.shape[0]
    shape = (m // 2, nd, HEAD, r) if aligned else arrived.shape
    keep, send = pl.pallas_call(
        lambda *a: recode_kernel(aligned, n, *a),
        out_shape=(jax.ShapeDtypeStruct(shape, bf16),) * 2,
        in_specs=[pl.BlockSpec(memory_space=pltpu.SMEM), vm, vm, vm],
        out_specs=(vm, vm),
        name="recode",
    )(where, arrived, mine, mean)
    if not aligned:
        pairs = jnp.bitwise_xor(where[1] // 2, jnp.arange(m // 2, dtype=jnp.int32))
        blocks = keep.reshape(nd, HEAD, m, r).transpose(2, 0, 1, 3)
        parity = where[1] % 2
        keep = jnp.take(blocks, pairs * 2 + parity, axis=0)
        send = jnp.take(blocks, pairs * 2 + 1 - parity, axis=0)
    return keep, send


def body(tokens, codes, scales, gain, cotangent):
    n = lax.axis_size("gx")
    m = lax.axis_size("gy")
    gi = lax.axis_index("gx")
    gj = lax.axis_index("gy")
    r = codes.shape[0]
    kv = codes.shape[1]
    heads = kv // HEAD
    nd = n // 2
    barrier = lax.optimization_barrier

    own = scaled(codes, scales)
    ra = r * 5 // 8 // 16 * 16
    shift = lambda x, s: lax.ppermute(x, "gx", [(i, (i + s) % n) for i in range(n)])
    flip = lambda x, mask: lax.ppermute(x, "gy", [(j, j ^ mask) for j in range(m)])
    part_a, part_b = own[:ra], own[ra:]
    near = [part_a] + [shift(part_a, s) for s in range(1, n)]
    far = [part_b] + [flip(part_b, s) for s in range(2, m, 2)]
    near, far = barrier((jnp.stack(near), jnp.stack(far)))
    near_all = [near] + [flip(near, s) for s in range(2, m, 2)]
    far_all = [far] + [shift(far, s) for s in range(1, n)]
    pieces = []
    for x in near_all + far_all:
        pieces += [x, flip(x, 1)]

    pm = signs(HEAD)
    had = jnp.asarray(pm, bf16)
    mean = jnp.asarray(block_mean_matrix(HEAD), bf16)
    side = jnp.where(gi < nd, 1, 0)
    where = jnp.stack([gi, gj, side]).astype(jnp.int32)
    keys, key_grad, qt, first0, weight = main_call(
        n, m, r, ra, where, tokens, gain.reshape(1, HEAD), cotangent, had, mean, pieces
    )

    hops = n - 1
    arrived = {}

    def hop(g, k, pay):
        arrived[g, k] = lax.ppermute(pay, "gx", [(g, g + 1), (n - 1 - g, n - 2 - g)])

    exchange = flip
    kept, met, parts, totals = {}, {}, {}, {}

    def phase_a(k):
        keep, send = recode_call(n, m, r, where, arrived[hops - 1, k], second[k], mean)
        kept[k] = keep
        met[k] = exchange(send, 1)

    def phase_b(k):
        whole = kept[k].astype(f32) + met[k].astype(f32)
        blocks = barrier(tuple([whole[0]] + [whole[x].astype(bf16) for x in range(1, m // 2)]))
        parts[k] = [blocks[0]]
        for x in range(1, m // 2):
            parts[k].append(exchange(blocks[x], 2 * x))

    def phase_c(k):
        total = parts[k][0]
        for x in parts[k][1:]:
            total = total + x.astype(f32)
        totals[k] = total

    def terms(is_first, skip, size):
        return list(term_call(n, m, r, where, tokens, qt, mean, is_first, skip, size))

    first = [first0] + terms(True, 1, 1) + terms(True, 2, heads - 2)
    second = terms(False, 0, heads)
    token_grad = None
    for part in range(TG_PARTS):
        token_grad = tgrad_call(key_grad, weight, token_grad, part, TG_PARTS)
    for k in range(heads):
        hop(0, k, first[k])
        for g in range(1, hops):
            hop(g, k, arrived[g - 1, k] + (first if g < nd else second)[k])
        phase_a(k)
        phase_b(k)
        phase_c(k)

    rotation = jnp.asarray(pm / np.float32(math.sqrt(HEAD)), f32)
    at_end = jnp.logical_or(gi == 0, gi == n - 1)
    out = []
    for batch in (list(range(heads - 1)), [heads - 1]):
        result = None
        for d in range(nd):
            value = jnp.stack([totals[k][d] for k in batch])
            if d == 0:
                value = jnp.where(at_end, value, 0.0)
            else:
                value = lax.ppermute(value.astype(bf16), "gx", [(0, d), (n - 1, n - 1 - d)]).astype(f32)
            result = value if result is None else result + value
        turned = jnp.einsum("har,ab->rhb", result, rotation, precision=HI)
        out.append(turned.reshape(r, len(batch) * HEAD))
    return keys, token_grad, jnp.concatenate(out, axis=1)


def solution(mesh):
    in_specs = (
        P(("gx", "gy"), None),
        P(("gx", "gy"), None),
        P(("gx", "gy"), None),
        P(),
        P(("gx", "gy"), None),
    )
    out_specs = (P(("gx", "gy"), None), P(("gx", "gy"), None), P(("gx", "gy"), None))

    return jax.shard_map(body, mesh=mesh, in_specs=in_specs, out_specs=out_specs, check_vma=False)
```

```python
import math

import jax
import jax.numpy as jnp
import numpy as np
from jax import lax
from jax.experimental import pallas as pl
from jax.experimental.pallas import tpu as pltpu
from jax.sharding import PartitionSpec as P


HEAD = 128
QBLK = 32
PARTS = 2
CLIP = 2.5
EPS = 1e-06


f32 = jnp.float32
bf16 = jnp.bfloat16
HI = lax.Precision.HIGHEST
BIG = pltpu.CompilerParams(vmem_limit_bytes=60 * 1024 * 1024)


def signs(length):
    idx = np.arange(length)
    common = idx[:, None] & idx[None, :]
    parity = np.zeros((length, length), np.int64)
    for pos in range(length.bit_length() - 1):
        parity += (common >> pos) & 1
    return (1 - 2 * (parity % 2)).astype(np.float32)


def block_mean_matrix(rows):
    lane = np.arange(128)
    return ((lane[:, None] // QBLK) == (lane[None, :] // QBLK)).astype(np.float32) / (QBLK * rows)


def three_parts(x):
    high = x.astype(bf16)
    rest = x - high.astype(f32)
    middle = rest.astype(bf16)
    low = (rest - middle.astype(f32)).astype(bf16)
    return jnp.concatenate([high, middle, low], axis=0)


def clipped_tiles(value, mean_matrix):
    heads = value.shape[0] // HEAD
    groups = value.shape[1] // 128
    tiles = [
        value[h * HEAD : (h + 1) * HEAD, g * 128 : (g + 1) * 128] for h in range(heads) for g in range(groups)
    ]
    rows = [jnp.sum(x * x, axis=0, keepdims=True) for x in tiles]
    pad = -len(rows) % 8
    if pad:
        rows.append(jnp.zeros((pad, 128), f32))
    squares = jnp.concatenate(rows, axis=0)
    count = squares.shape[0]
    parts = jnp.dot(three_parts(squares), mean_matrix, preferred_element_type=f32)
    means = parts[:count] + parts[count : 2 * count] + parts[2 * count :]
    bounds = CLIP * jnp.sqrt(means + EPS)
    for at, x in enumerate(tiles):
        limit = bounds[at : at + 1]
        yield at // groups, at % groups, jnp.minimum(jnp.maximum(x, -limit), limit).astype(bf16)


def scale_kernel(scales_ref, codes_ref, out_ref):
    blocks = codes_ref.shape[0] // QBLK
    heads = codes_ref.shape[1] // HEAD
    for b in range(blocks):
        for h in range(heads):
            tile = codes_ref[b * QBLK : (b + 1) * QBLK, h * HEAD : (h + 1) * HEAD].astype(f32)
            out_ref[b * QBLK : (b + 1) * QBLK, h * HEAD : (h + 1) * HEAD] = (tile * scales_ref[b, h]).astype(bf16)


def scaled(codes, scales):
    return pl.pallas_call(
        scale_kernel,
        out_shape=jax.ShapeDtypeStruct(codes.shape, bf16),
        in_specs=[pl.BlockSpec(memory_space=pltpu.SMEM), pl.BlockSpec(memory_space=pltpu.VMEM)],
        out_specs=pl.BlockSpec(memory_space=pltpu.VMEM),
        name="scale_rows",
    )(scales, codes)


def piece_copies(n, m, r, x, where_ref, tok_hbm, parts, tv, wv, sem):
    gi, pair, parity = where_ref[0], where_ref[1] // 2, lax.rem(where_ref[1], 2)
    copies = []
    size = r // PARTS

    def add(source, target):
        copies.append(pltpu.make_async_copy(source, target, sem.at[len(copies)]))

    for a in range(n):
        col = (lax.rem(gi - a + n, n) * (m // 2) + jnp.bitwise_xor(pair, x)) * (2 * r)
        for p in range(PARTS):
            for flipped in range(2):
                row = 2 * a * r + jnp.where(parity == flipped, 0, r) + p * size
                add(parts[2 * p + flipped].at[a], wv.at[pl.ds(pl.multiple_of(row, 16), size)])
        add(tok_hbm.at[:, pl.ds(pl.multiple_of(col, 128), 2 * r)], tv.at[:, pl.ds(a * 2 * r, 2 * r)])
    for c in copies:
        c.start()
    return copies


def gather_dot_kernel(n, m, r, where_ref, tok_hbm, *refs):
    parts = refs[: 2 * PARTS]
    acc_ref, w_ref, tv, sem = refs[2 * PARTS :]
    for c in piece_copies(n, m, r, 0, where_ref, tok_hbm, parts, tv, w_ref, sem):
        c.wait()
    acc_ref[...] = jnp.dot(tv[...], w_ref[...], preferred_element_type=f32)


def gather_dot(n, m, r, where, tokens, parts):
    tok = tokens.shape[0]
    kv = parts[0].shape[-1]
    vm = pl.BlockSpec(memory_space=pltpu.VMEM)
    hbm = pl.BlockSpec(memory_space=pltpu.HBM)
    rows = n * 2 * r
    return pl.pallas_call(
        lambda *a: gather_dot_kernel(n, m, r, *a),
        out_shape=(jax.ShapeDtypeStruct((tok, kv), f32), jax.ShapeDtypeStruct((rows, kv), bf16)),
        in_specs=[pl.BlockSpec(memory_space=pltpu.SMEM), hbm] + [hbm] * len(parts),
        out_specs=(vm, vm),
        scratch_shapes=[pltpu.VMEM((tok, rows), bf16), pltpu.SemaphoreType.DMA((n * (2 * PARTS + 1),))],
        compiler_params=BIG,
        name="gather_dot",
    )(where, tokens, *parts)


def norm_kernel(n, m, r, xs, where_ref, tok_hbm, gain_ref, cot_ref, had_ref, mean_ref, acc_ref, *refs):
    heads = cot_ref.shape[1] // HEAD
    count = len(xs)
    parts, refs = refs[: 2 * PARTS * count], refs[2 * PARTS * count :]
    keys_ref, kg_ref, qt_ref = refs[:3]
    term_refs, refs = refs[3 : 3 + heads], refs[3 + heads :]
    w_refs, refs = refs[:count], refs[count:]
    fv, fsem, refs = refs[0], refs[1], refs[2:]
    side = where_ref[2]
    width = m * r
    nd = n // 2
    start = pl.multiple_of(jnp.where(side == 0, 0, n - nd) * width, 128)
    batches = []
    for p, x in enumerate(xs):
        mine = parts[2 * PARTS * p : 2 * PARTS * (p + 1)]
        batches.append(
            piece_copies(n, m, r, x, where_ref, tok_hbm, mine, refs[2 + p], w_refs[p], refs[0].at[p])
        )
    half = pltpu.make_async_copy(tok_hbm.at[:, pl.ds(start, nd * width)], fv, fsem)
    half.start()
    acc = refs[1] if count else acc_ref
    for p, batch in enumerate(batches):
        for c in batch:
            c.wait()
        base = acc if p else acc_ref
        acc[...] = base[...] + jnp.dot(refs[2 + p][...], w_refs[p][...], preferred_element_type=f32)
    gain = gain_ref[...]
    for h in range(heads):
        lanes = slice(h * HEAD, (h + 1) * HEAD)
        raw = acc[:, lanes]
        inv = lax.rsqrt(jnp.mean(raw * raw, axis=-1, keepdims=True) + EPS)
        unit = raw * inv
        keys_ref[:, lanes] = (unit * gain).astype(bf16)
        g = cot_ref[:, lanes].astype(f32) * gain
        kg = (inv * (g - unit * jnp.mean(g * unit, axis=-1, keepdims=True))).astype(bf16)
        kg_ref[:, lanes] = kg
        turned = lax.dot_general(had_ref[...], kg, (((1,), (1,)), ((), ())), preferred_element_type=f32)
        qt_ref[lanes, :] = (turned * (1.0 / math.sqrt(HEAD))).astype(bf16)
    half.wait()
    bw = min(width, 512)
    for d in range(nd):
        row = jnp.where(side == 0, d, nd - 1 - d)
        for b in range(width // bw):
            off = pl.multiple_of(row * width + b * bw, bw)
            value = jnp.dot(qt_ref[...], fv[:, pl.ds(off, bw)], preferred_element_type=f32)
            for h, g, y in clipped_tiles(value, mean_ref[...]):
                term_refs[h][d, :, b * bw + g * 128 : b * bw + (g + 1) * 128] = y


def norm_call(n, m, r, xs, where, tokens, gain, cot, had, mean, acc, parts):
    tok = tokens.shape[0]
    kv = acc.shape[1]
    heads = kv // HEAD
    nd = n // 2
    rows = n * 2 * r
    count = len(xs)
    vm = pl.BlockSpec(memory_space=pltpu.VMEM)
    hbm = pl.BlockSpec(memory_space=pltpu.HBM)
    shapes = [
        jax.ShapeDtypeStruct((tok, kv), bf16),
        jax.ShapeDtypeStruct((tok, kv), bf16),
        jax.ShapeDtypeStruct((kv, tok), bf16),
    ]
    shapes += [jax.ShapeDtypeStruct((nd, HEAD, m * r), bf16)] * heads
    shapes += [jax.ShapeDtypeStruct((rows, kv), bf16)] * count
    scratch = [pltpu.VMEM((tok, nd * m * r), bf16), pltpu.SemaphoreType.DMA]
    if count:
        scratch += [pltpu.SemaphoreType.DMA((count, n * (2 * PARTS + 1))), pltpu.VMEM((tok, kv), f32)]
        scratch += [pltpu.VMEM((tok, rows), bf16)] * count
    return pl.pallas_call(
        lambda *a: norm_kernel(n, m, r, xs, *a),
        out_shape=shapes,
        in_specs=[pl.BlockSpec(memory_space=pltpu.SMEM), hbm] + [vm] * 5 + [hbm] * len(parts),
        out_specs=[vm] * len(shapes),
        scratch_shapes=scratch,
        compiler_params=BIG,
        name="norm",
    )(where, tokens, gain, cot, had, mean, acc, *parts)


def term_kernel(groups, where_ref, tok_ref, *refs):
    mean_ref, out_refs = refs[groups], refs[groups + 1 :]
    at = 0
    for qt_ref in refs[:groups]:
        value = jnp.dot(qt_ref[...], tok_ref[...], preferred_element_type=f32)
        for h, g, x in clipped_tiles(value, mean_ref[...]):
            out_refs[at + h][0, :, g * 128 : (g + 1) * 128] = x
        at += qt_ref.shape[0] // HEAD


def term_call(n, m, r, where, tokens, qts, mean):
    tok = tokens.shape[0]
    rows = [q.shape[0] for q in qts]
    heads = sum(rows) // HEAD
    nd = n // 2
    width = m * r
    bw = min(1024, width)
    nb = width // bw

    def tok_index(d, b, where_ref):
        row = jnp.where(where_ref[2] == 0, n - 1 - d, d)
        return (0, row * nb + b)

    return pl.pallas_call(
        lambda *a: term_kernel(len(qts), *a),
        grid_spec=pltpu.PrefetchScalarGridSpec(
            num_scalar_prefetch=1,
            grid=(nd, nb),
            in_specs=[pl.BlockSpec((tok, bw), tok_index)]
            + [pl.BlockSpec((size, tok), lambda d, b, w: (0, 0)) for size in rows]
            + [pl.BlockSpec((128, 128), lambda d, b, w: (0, 0))],
            out_specs=[pl.BlockSpec((1, HEAD, bw), lambda d, b, w: (d, 0, b))] * heads,
        ),
        out_shape=[jax.ShapeDtypeStruct((nd, HEAD, width), bf16)] * heads,
        compiler_params=BIG,
        name="terms",
    )(where, tokens, *qts, mean)


def tgrad_kernel(n, m, r, xs, where_ref, kg_ref, *refs):
    out_hbm, slabs, sem = refs[-3:]
    gi, pair = where_ref[0], where_ref[1] // 2
    copies = []
    for p, x in enumerate(xs):
        for a in range(n):
            at = p * n + a
            col = (lax.rem(gi - a + n, n) * (m // 2) + jnp.bitwise_xor(pair, x)) * (2 * r)
            slabs[at] = lax.dot_general(
                kg_ref[...], refs[p][a * 2 * r : (a + 1) * 2 * r], (((1,), (1,)), ((), ())),
                preferred_element_type=f32,
            ).astype(bf16)
            copy = pltpu.make_async_copy(
                slabs.at[at], out_hbm.at[:, pl.ds(pl.multiple_of(col, 128), 2 * r)], sem.at[at]
            )
            copy.start()
            copies.append(copy)
    for c in copies:
        c.wait()


def tgrad_call(n, m, r, xs, where, kg, weights, filled, d_model):
    tok = kg.shape[0]
    vm = pl.BlockSpec(memory_space=pltpu.VMEM)
    hbm = pl.BlockSpec(memory_space=pltpu.HBM)
    extra = [] if filled is None else [filled]
    count = n * len(xs)
    return pl.pallas_call(
        lambda *a: tgrad_kernel(n, m, r, xs, *a),
        in_specs=[pl.BlockSpec(memory_space=pltpu.SMEM)] + [vm] * (1 + len(xs)) + [hbm] * len(extra),
        out_specs=hbm,
        out_shape=jax.ShapeDtypeStruct((tok, d_model), bf16),
        scratch_shapes=[pltpu.VMEM((count, tok, 2 * r), bf16), pltpu.SemaphoreType.DMA((count,))],
        input_output_aliases={2 + len(xs): 0} if extra else {},
        compiler_params=BIG,
        name="token_grad",
    )(where, kg, *weights, *extra)


def recode_kernel(aligned, n, where_ref, a_ref, b_ref, mean_ref, keep_ref, send_ref):
    pair, parity = where_ref[1] // 2, lax.rem(where_ref[1], 2)

    @pl.when(jnp.logical_or(where_ref[0] == 0, where_ref[0] == n - 1))
    def _():
        for d in range(a_ref.shape[0]):
            value = a_ref[d].astype(f32) + b_ref[d].astype(f32)
            tiles = [x for _, _, x in clipped_tiles(value, mean_ref[...])]
            for g, x in enumerate(tiles):
                if not aligned:
                    keep_ref[d, :, g * 128 : (g + 1) * 128] = x
                elif g % 2 == 0:
                    at = jnp.bitwise_xor(pair, g // 2)
                    keep_ref[at, d] = jnp.where(parity == 0, x, tiles[g + 1])
                    send_ref[at, d] = jnp.where(parity == 0, tiles[g + 1], x)


def recode_call(n, m, r, where, arrived, mine, mean):
    aligned = r == 128
    vm = pl.BlockSpec(memory_space=pltpu.VMEM)
    nd = arrived.shape[0]
    shape = (m // 2, nd, HEAD, r) if aligned else arrived.shape
    keep, send = pl.pallas_call(
        lambda *a: recode_kernel(aligned, n, *a),
        out_shape=(jax.ShapeDtypeStruct(shape, bf16),) * 2,
        in_specs=[pl.BlockSpec(memory_space=pltpu.SMEM), vm, vm, vm],
        out_specs=(vm, vm),
        name="recode",
    )(where, arrived, mine, mean)
    if not aligned:
        pairs = jnp.bitwise_xor(where[1] // 2, jnp.arange(m // 2, dtype=jnp.int32))
        blocks = keep.reshape(nd, HEAD, m, r).transpose(2, 0, 1, 3)
        parity = where[1] % 2
        keep = jnp.take(blocks, pairs * 2 + parity, axis=0)
        send = jnp.take(blocks, pairs * 2 + 1 - parity, axis=0)
    return keep, send


def body(tokens, codes, scales, gain, cotangent):
    n = lax.axis_size("gx")
    m = lax.axis_size("gy")
    gi = lax.axis_index("gx")
    gj = lax.axis_index("gy")
    r = codes.shape[0]
    kv = codes.shape[1]
    heads = kv // HEAD
    nd = n // 2
    barrier = lax.optimization_barrier

    _, d_model = tokens.shape
    pm = signs(HEAD)
    had = jnp.asarray(pm, bf16)
    mean = jnp.asarray(block_mean_matrix(HEAD), bf16)
    side = jnp.where(gi < nd, 1, 0)
    where = jnp.stack([gi, gj, side]).astype(jnp.int32)
    aligned = 2 * r % 128 == 0 and m == 8

    flip = lambda x, mask: lax.ppermute(x, "gy", [(j, j ^ mask) for j in range(m)])
    own = scaled(codes, scales)
    size = r // PARTS
    pieces = [[] for _ in range(m // 2)]
    for p in range(PARTS):
        mine = own[p * size : (p + 1) * size]
        near = [mine]
        for s in range(1, n):
            near.append(lax.ppermute(mine, "gx", [(i, (i + s) % n) for i in range(n)]))
        near = jnp.stack(near)
        for x in range(m // 2):
            piece = near
            if x:
                piece = flip(near, 2 * x)
            pieces[x] += [piece, flip(piece, 1)]
    norm_args = (where, tokens, gain.reshape(1, HEAD), cotangent, had, mean)
    if aligned:
        acc, w0 = gather_dot(n, m, r, where, tokens, pieces[0])
        keys, key_grad, qt, *first, w1, w2, w3 = norm_call(
            n, m, r, (1, 2, 3), *norm_args, acc, pieces[1] + pieces[2] + pieces[3]
        )
        weights = [w0, w1, w2, w3]
    else:
        rows = [jnp.concatenate(piece[q::2], axis=1) for piece in pieces for q in range(2)]
        block = jnp.stack(rows)
        block = jnp.take(block, jnp.bitwise_xor(gj, jnp.arange(m, dtype=jnp.int32)), axis=0)
        block = jnp.take(block, (gi - jnp.arange(n, dtype=jnp.int32)) % n, axis=1)
        weight = block.transpose(1, 0, 2, 3).reshape(d_model, kv)
        acc = jnp.dot(tokens, weight, preferred_element_type=f32)
        keys, key_grad, qt, *first = norm_call(n, m, r, (), *norm_args, acc, [])

    hops = n - 1
    arrived = {}

    def hop(g, k, pay):
        arrived[g, k] = lax.ppermute(pay, "gx", [(g, g + 1), (n - 1 - g, n - 2 - g)])

    exchange = flip
    kept, met, totals = {}, {}, {}

    def phase_a(k):
        keep, send = recode_call(n, m, r, where, arrived[hops - 1, k], second[k], mean)
        kept[k] = keep
        met[k] = exchange(send, 1)

    def phase_b(group):
        sums = [kept[k].astype(f32) + met[k].astype(f32) for k in group]
        join = lambda x: jnp.concatenate([w[x] for w in sums])
        blocks = barrier(tuple([join(0)] + [join(x).astype(bf16) for x in range(1, m // 2)]))
        total = blocks[0]
        for x in range(1, m // 2):
            total = total + exchange(blocks[x], 2 * x).astype(f32)
        for at, k in enumerate(group):
            totals[k] = total[at * nd : (at + 1) * nd]

    second = term_call(n, m, r, where, tokens, [qt], mean)
    token_grad = None
    if aligned:
        for xs in ((0, 1), (2,), (3,)):
            token_grad = tgrad_call(
                n, m, r, xs, where, key_grad, [weights[x] for x in xs], token_grad, d_model
            )
    else:
        token_grad = lax.dot_general(
            key_grad, weight, (((1,), (1,)), ((), ())), preferred_element_type=f32
        ).astype(bf16)
    for k in range(heads):
        hop(0, k, first[k])
        for g in range(1, hops):
            hop(g, k, arrived[g - 1, k] + (first if g < nd else second)[k])
        phase_a(k)
    for group in (list(range(heads - 2)), [heads - 2], [heads - 1]):
        phase_b(group)

    rotation = jnp.asarray(pm / np.float32(math.sqrt(HEAD)), f32)
    at_end = jnp.logical_or(gi == 0, gi == n - 1)
    out = []
    for batch in (list(range(heads)),):
        result = None
        for d in range(nd):
            value = jnp.stack([totals[k][d] for k in batch])
            if d == 0:
                value = jnp.where(at_end, value, 0.0)
            else:
                value = lax.ppermute(value.astype(bf16), "gx", [(0, d), (n - 1, n - 1 - d)]).astype(f32)
            result = value if result is None else result + value
        turned = jnp.einsum("har,ab->rhb", result, rotation, precision=HI)
        out.append(turned.reshape(r, len(batch) * HEAD))
    return keys, token_grad, jnp.concatenate(out, axis=1)


def solution(mesh):
    in_specs = (
        P(("gx", "gy"), None),
        P(("gx", "gy"), None),
        P(("gx", "gy"), None),
        P(),
        P(("gx", "gy"), None),
    )
    out_specs = (P(("gx", "gy"), None), P(("gx", "gy"), None), P(("gx", "gy"), None))

    return jax.shard_map(body, mesh=mesh, in_specs=in_specs, out_specs=out_specs, check_vma=False)
```
